32 devices in a mesh: surf: 32 (over z, y, x, core).
Axes of the slice: x: 2, y: 2, z: 4, core: 2. Of those that a mesh axis runs over, the one named last changes fastest.
Arguments:
- excitation: float32 [2, 16384, 256], P(None, 'surf'), may hold values from -6 to 6
- leaf_basis: bfloat16 [2, 8192, 512], P(None, 'surf'), may hold values from -0.1875 to 0.1875
- self_transfer: bfloat16 [3, 2, 8192, 256], P(None, None, 'surf'), may hold values from -0.1875 to 0.1875
- cross_transfer: bfloat16 [3, 2, 8192, 256], P(None, None, 'surf'), may hold values from -0.1875 to 0.1875
- out_basis: bfloat16 [2, 16384, 256], P(None, 'surf'), may hold values from -0.25 to 0.25
- near_tiles: bfloat16 [192, 2, 128, 128], P('surf'), may hold values from -0.375 to 0.375
- near_list: int32 [32, 6, 3], replicated, may hold values from -1 to 31, as said below
Outputs:
- response: float32 [2, 16384, 256], P(None, 'surf')
The draws below stay inside these ranges and needn't reach their ends.
Inputs may be any that keep to these rules, and one draw needn't show every extreme that they name: `near_list`: row i lists patch i's near tiles as (owner, row tile, column tile). An owner is i - 1, i or i + 1 modulo 32, or -1 for an empty slot; empty slots come last and hold 0 for both tiles. Every patch has at least one tile and some patch fills all 6 slots. From one neighbouring patch a patch lists at most 2 distinct column tiles, and some patch reaches 2.
All inputs are finite; a program needn't handle non-finite values.
Results may differ from the reference program's by a relative error of at most 0.0051.
Values may be sent and summed in bfloat16 or wider, within the bound.
No kernel may reach another device: no remote copies, remote signals or barrier semaphores. Data moves between devices by JAX's collectives and lax.ppermute only.
A program may use at most 64 MiB of HBM per device.

```python
import jax
import jax.numpy as jnp
from jax import lax

TILE = 128
PATCH_ROW_TILES = 4
RANK = 256
COLS = 256
BUTTERFLY_DEPTH = 3
NEAR_TILE_SLOTS = 6
ROWS = 512
ORDER = 16384
N_SURF = 32


def draw_near_list(key, part):
    random_keys = jax.random.split(jax.random.fold_in(key, 71), 7)
    processor_index = jnp.arange(N_SURF, dtype=jnp.int32)[:, None]
    transfer_group = jax.random.randint(random_keys[0], (N_SURF,), 0, 8) == 0
    tile_count = jnp.where(transfer_group, NEAR_TILE_SLOTS, jax.random.randint(random_keys[1], (N_SURF,), min(4, NEAR_TILE_SLOTS), NEAR_TILE_SLOTS + 1))
    tile_count = tile_count.at[0].set(NEAR_TILE_SLOTS)
    first = jax.random.randint(random_keys[2], (N_SURF, 3), 0, PATCH_ROW_TILES)
    second = (first + jax.random.randint(random_keys[3], (N_SURF, 3), 1, PATCH_ROW_TILES)) % PATCH_ROW_TILES
    draw_side = jax.random.randint(random_keys[4], (N_SURF, NEAR_TILE_SLOTS), 0, 5)
    side = jnp.where(draw_side < 2, 0, jnp.where(draw_side == 2, 1, 2))
    side = side.at[0, 0].set(2).at[0, 1].set(2)
    pick = jax.random.randint(random_keys[5], (N_SURF, NEAR_TILE_SLOTS), 0, 2)
    pick = pick.at[0, 0].set(0).at[0, 1].set(1)
    column = jnp.where(pick == 0, jnp.take_along_axis(first, side, 1), jnp.take_along_axis(second, side, 1))
    row_tile = jax.random.randint(random_keys[6], (N_SURF, NEAR_TILE_SLOTS), 0, PATCH_ROW_TILES)
    owner = (processor_index + side - 1) % N_SURF
    live = jnp.arange(NEAR_TILE_SLOTS)[None, :] < tile_count[:, None]
    owner = jnp.where(live, owner, -1)
    row_tile = jnp.where(live, row_tile, 0)
    column = jnp.where(live, column, 0)
    return jnp.stack([owner, row_tile, column], -1).astype(jnp.int32)


def block_levels(rng, shape, cuts, smallest, high):
    def one(dim, parts):
        steps = jax.random.uniform(jax.random.fold_in(jax.random.fold_in(rng, 6), dim), (parts,), jnp.float32, smallest / len(cuts), high / len(cuts))
        return jnp.repeat(jnp.exp(steps), shape[dim] // parts).reshape((-1,) + (1,) * (len(shape) - dim - 1))

    factor_of = one(*cuts[0])
    for cut in cuts[1:]:
        factor_of = factor_of * one(*cut)
    return factor_of


def bell_draw(rng, shape, spread, limit, cuts=(), kind=jnp.bfloat16):
    level = block_levels(rng, shape, cuts, -0.22, 0.18) if cuts else 1.0
    drawn = jax.random.normal(rng, shape, jnp.float32) * spread * level
    return jnp.minimum(jnp.maximum(drawn, -limit), limit).astype(kind)


def setup_inputs(seed: int = 0) -> dict:
    splits = jax.random.split(jax.random.key(seed), 8)
    excitation = bell_draw(splits[0], (2, ORDER, COLS), 1.0, 6.0, ((1, 32),), jnp.float32)
    leaf_basis = bell_draw(splits[1], (2, RANK * N_SURF, ROWS), (2 * ROWS) ** -0.5, 0.1875, ((1, 32),))
    self_transfer = bell_draw(splits[2], (BUTTERFLY_DEPTH, 2, RANK * N_SURF, RANK), (4 * RANK) ** -0.5, 0.1875, ((2, 32),))
    cross_transfer = bell_draw(splits[3], (BUTTERFLY_DEPTH, 2, RANK * N_SURF, RANK), (4 * RANK) ** -0.5, 0.1875, ((2, 32),))
    out_basis = bell_draw(splits[4], (2, ORDER, RANK), (2 * RANK) ** -0.5, 0.25, ((1, 32),))
    near_tiles = bell_draw(splits[5], (N_SURF * NEAR_TILE_SLOTS, 2, TILE, TILE), (2 * TILE) ** -0.5, 0.375, ((0, 32),))
    near_list = draw_near_list(jax.random.fold_in(splits[7], 71), 0)
    return dict(excitation=excitation, leaf_basis=leaf_basis, self_transfer=self_transfer, cross_transfer=cross_transfer, out_basis=out_basis, near_tiles=near_tiles, near_list=near_list)


def cmat(matrix, vector):
    real = jnp.dot(matrix[0], vector[0], preferred_element_type=jnp.float32) - jnp.dot(matrix[1], vector[1], preferred_element_type=jnp.float32)
    imag = jnp.dot(matrix[0], vector[1], preferred_element_type=jnp.float32) + jnp.dot(matrix[1], vector[0], preferred_element_type=jnp.float32)
    return jnp.stack([real, imag])


def per_patch(array, inner, last):
    return array.reshape(2, N_SURF, inner, last).transpose(1, 0, 2, 3)


def reference(excitation, leaf_basis, self_transfer, cross_transfer, out_basis, near_tiles, near_list):
    xb = excitation.astype(jnp.bfloat16)
    patches = per_patch(xb, ROWS, COLS)
    leaves = per_patch(leaf_basis, RANK, ROWS)
    coef = lax.map(lambda pair: cmat(pair[0], pair[1]).astype(jnp.bfloat16), (leaves, patches))
    idents = jnp.arange(N_SURF, dtype=jnp.int32)
    for level in range(BUTTERFLY_DEPTH):
        exchange_partner = coef[jnp.bitwise_xor(idents, 1 << level)]
        own_maps = per_patch(self_transfer[level], RANK, RANK)
        far_maps = per_patch(cross_transfer[level], RANK, RANK)
        coef = lax.map(lambda quad: (cmat(quad[0], quad[1]) + cmat(quad[2], quad[3])).astype(jnp.bfloat16), (own_maps, coef, far_maps, exchange_partner))
    outs = per_patch(out_basis, ROWS, RANK)
    far = lax.map(lambda pair: cmat(pair[0], pair[1]), (outs, coef))
    tiles = near_tiles.reshape(N_SURF, NEAR_TILE_SLOTS, 2, TILE, TILE)
    block_ids = jnp.arange(PATCH_ROW_TILES, dtype=jnp.int32)

    def near_one(pair):
        tile_set, listing = pair
        near = jnp.zeros((2, PATCH_ROW_TILES, TILE, COLS), jnp.float32)
        for slot in range(NEAR_TILE_SLOTS):
            owner = listing[slot, 0]
            valid = (owner >= 0).astype(jnp.float32)
            start = (jnp.maximum(owner, 0) * ROWS + listing[slot, 2] * TILE).astype(jnp.int32)
            block = lax.dynamic_slice_in_dim(xb, start, TILE, 1)
            term = cmat(tile_set[slot], block) * valid
            hit = (block_ids == listing[slot, 1].astype(jnp.int32)).astype(jnp.float32)
            near = near + term[:, None] * hit[None, :, None, None]
        return near.reshape(2, ROWS, COLS)

    near = lax.map(near_one, (tiles, near_list))
    total = far + near
    return total.transpose(1, 0, 2, 3).reshape(2, N_SURF * ROWS, COLS)
```

```python
import functools

import jax
import jax.numpy as jnp
from jax import lax
from jax.experimental import pallas as pl
from jax.experimental.pallas import tpu as pltpu
from jax.sharding import PartitionSpec as P

CHUNKS = 2
VMEM_LIMIT = 12 * 1024 * 1024

ON_CHIP = pl.BlockSpec(memory_space=pltpu.VMEM)
SCALARS = pl.BlockSpec(memory_space=pltpu.SMEM)


def call(body, name, outs, ins, args, flops, nbytes, scratch=()):
    return pl.pallas_call(
        body,
        name=name,
        out_shape=outs,
        in_specs=ins,
        out_specs=[ON_CHIP] * len(outs),
        scratch_shapes=list(scratch),
        cost_estimate=pl.CostEstimate(
            flops=flops, bytes_accessed=nbytes, transcendentals=0
        ),
        compiler_params=pltpu.CompilerParams(vmem_limit_bytes=VMEM_LIMIT),
    )(*args)


def dot(a, b):
    return jnp.dot(a, b, preferred_element_type=jnp.float32)


def complex_dot(m0, m1, v0, v1):
    return dot(m0, v0) - dot(m1, v1), dot(m0, v1) + dot(m1, v0)


def leaf_body(x_ref, leaf_ref, xb_ref, *coef_refs):
    xb_ref[...] = x_ref[...].astype(jnp.bfloat16)
    width = coef_refs[0].shape[2]
    for c, ref in enumerate(coef_refs):
        cols = slice(c * width, (c + 1) * width)
        real, imag = complex_dot(
            leaf_ref[0], leaf_ref[1], xb_ref[0, :, cols], xb_ref[1, :, cols]
        )
        ref[0] = real.astype(ref.dtype)
        ref[1] = imag.astype(ref.dtype)


def span(list_ref, reader, owner, blocks):
    low = jnp.int32(blocks - 1)
    high = jnp.int32(0)
    for slot in range(list_ref.shape[0]):
        mine = list_ref[slot, 0, reader] == owner
        column = list_ref[slot, 2, reader]
        low = jnp.minimum(low, jnp.where(mine, column, low))
        high = jnp.maximum(high, jnp.where(mine, column, high))
    return low, high


def pick_body(axis, count, list_ref, xb_ref, up_ref, down_ref):
    tile = up_ref.shape[2]
    blocks = xb_ref.shape[1] // tile
    here = lax.axis_index(axis)
    for step, ref in ((1, up_ref), (count - 1, down_ref)):
        reader = lax.rem(here + step, count)
        for k, column in enumerate(span(list_ref, reader, here, blocks)):
            rows = pl.ds(pl.multiple_of(column * tile, tile), tile)
            ref[k] = xb_ref[:, rows, :]


def own_body(level, coef_ref, self_ref, out_ref):
    real, imag = complex_dot(
        self_ref[level, 0], self_ref[level, 1], coef_ref[0], coef_ref[1]
    )
    out_ref[0] = real
    out_ref[1] = imag


def cross_body(level, own_ref, partner_ref, cross_ref, out_ref):
    real, imag = complex_dot(
        cross_ref[level, 0], cross_ref[level, 1], partner_ref[0], partner_ref[1]
    )
    out_ref[0] = (own_ref[0] + real).astype(out_ref.dtype)
    out_ref[1] = (own_ref[1] + imag).astype(out_ref.dtype)


def near_body(axis, count, list_ref, tiles_ref, xb_ref, low_ref, high_ref, near_ref):
    tile = tiles_ref.shape[2]
    blocks = xb_ref.shape[1] // tile
    here = lax.axis_index(axis)
    before = lax.rem(here + count - 1, count)
    after = lax.rem(here + 1, count)
    low_first, _ = span(list_ref, here, before, blocks)
    high_first, _ = span(list_ref, here, after, blocks)
    near_ref[...] = jnp.zeros_like(near_ref)

    def add(slot, row, v0, v1):
        real, imag = complex_dot(tiles_ref[slot, 0], tiles_ref[slot, 1], v0, v1)
        rows = pl.ds(pl.multiple_of(row * tile, tile), tile)
        near_ref[0, rows, :] += real
        near_ref[1, rows, :] += imag

    for slot in range(tiles_ref.shape[0]):
        owner = list_ref[slot, 0, here]
        row = list_ref[slot, 1, here]
        column = list_ref[slot, 2, here]

        @pl.when(owner == here)
        def _():
            rows = pl.ds(pl.multiple_of(column * tile, tile), tile)
            add(slot, row, xb_ref[0, rows, :], xb_ref[1, rows, :])

        @pl.when(jnp.logical_and(owner >= 0, owner != here))
        def _():
            below = owner == before
            first = jnp.where(below, low_first, high_first)
            k = jnp.where(column == first, 0, 1)

            @pl.when(below)
            def _():
                add(slot, row, low_ref[k, 0], low_ref[k, 1])

            @pl.when(jnp.logical_not(below))
            def _():
                add(slot, row, high_ref[k, 0], high_ref[k, 1])


def last_body(level, *refs):
    *chunks, cross_ref, out_basis_ref, near_ref, out_ref = refs
    pieces = len(chunks) // 2
    for c in range(pieces):
        own_ref, partner_ref = chunks[c], chunks[pieces + c]
        width = partner_ref.shape[2]
        real, imag = complex_dot(
            cross_ref[level, 0], cross_ref[level, 1], partner_ref[0], partner_ref[1]
        )
        v0 = (own_ref[0] + real).astype(jnp.bfloat16)
        v1 = (own_ref[1] + imag).astype(jnp.bfloat16)
        real, imag = complex_dot(out_basis_ref[0], out_basis_ref[1], v0, v1)
        cols = slice(c * width, (c + 1) * width)
        out_ref[0, :, cols] = real + near_ref[0, :, cols]
        out_ref[1, :, cols] = imag + near_ref[1, :, cols]


def per_device(
    excitation, leaf_basis, self_transfer, cross_transfer, out_basis, near_tiles, near_list
):
    axis = "surf"
    count = lax.axis_size(axis)
    rows, width = excitation.shape[1:]
    rank = leaf_basis.shape[1]
    tile = near_tiles.shape[2]
    levels = self_transfer.shape[0]
    part = width // CHUNKS
    listing = near_list.transpose(1, 2, 0)
    up = [(i, (i + 1) % count) for i in range(count)]
    down = [(i, (i - 1) % count) for i in range(count)]
    piece = pltpu.VMEM((2, rank, part), jnp.bfloat16)
    total = pltpu.VMEM((2, rank, part), jnp.float32)

    xb, *coef = call(
        leaf_body,
        "leaf",
        [pltpu.VMEM(excitation.shape, jnp.bfloat16)] + [piece] * CHUNKS,
        [ON_CHIP, ON_CHIP],
        (excitation, leaf_basis),
        8 * rank * rows * width,
        8 * rows * width,
    )
    near = None
    for level in range(levels):
        swap = [(i, i ^ (1 << level)) for i in range(count)]
        partner = [lax.ppermute(c, axis, swap) for c in coef]
        if level == 0:
            sent = pltpu.VMEM((2, 2, tile, width), jnp.bfloat16)
            to_up, to_down = call(
                functools.partial(pick_body, axis, count),
                "pick",
                [sent, sent],
                [SCALARS, ON_CHIP],
                (listing, xb),
                0,
                8 * tile * width,
            )
            low = lax.ppermute(to_up, axis, up)
            high = lax.ppermute(to_down, axis, down)
        own = [
            call(
                functools.partial(own_body, level),
                "own",
                [total],
                [ON_CHIP, ON_CHIP],
                (c, self_transfer),
                8 * rank * rank * part,
                2 * rank * rank,
            )[0]
            for c in coef
        ]
        if level == levels - 1:
            (near,) = call(
                functools.partial(near_body, axis, count),
                "near",
                [pltpu.VMEM((2, rows, width), jnp.float32)],
                [SCALARS] + [ON_CHIP] * 4,
                (listing, near_tiles, xb, low, high),
                8 * near_tiles.shape[0] * tile * tile * width,
                8 * rows * width,
            )
            break
        coef = [
            call(
                functools.partial(cross_body, level),
                "cross",
                [piece],
                [ON_CHIP] * 3,
                (own[c], partner[c], cross_transfer),
                8 * rank * rank * part,
                2 * rank * rank,
            )[0]
            for c in range(CHUNKS)
        ]
    return call(
        functools.partial(last_body, levels - 1),
        "last",
        [jax.ShapeDtypeStruct((2, rows, width), jnp.float32)],
        [ON_CHIP] * (2 * CHUNKS + 3),
        (*own, *partner, cross_transfer, out_basis, near),
        8 * rank * (rank + rows) * width,
        8 * rows * width,
    )[0]


def solution(mesh):
    placed = (
        P(None, "surf", None),
        P(None, "surf", None),
        P(None, None, "surf", None),
        P(None, None, "surf", None),
        P(None, "surf", None),
        P("surf", None, None, None),
        P(),
    )
    return jax.shard_map(
        per_device, mesh=mesh, in_specs=placed, out_specs=P(None, "surf", None), check_vma=False
    )
```

```python
import functools

import jax
import jax.numpy as jnp
from jax import lax
from jax.experimental import pallas as pl
from jax.experimental.pallas import tpu as pltpu
from jax.sharding import PartitionSpec as P


CHUNKS = 2
VMEM_LIMIT = 12 * 1024 * 1024

ON_CHIP = pl.BlockSpec(memory_space=pltpu.VMEM)
OFF_CHIP = pl.BlockSpec(memory_space=pltpu.HBM)
SCALARS = pl.BlockSpec(memory_space=pltpu.SMEM)


def call(body, outs, ins, args, flops, nbytes, scratch=(), outs_at=None, aliases=None):
    return pl.pallas_call(
        body,
        out_shape=outs,
        in_specs=ins,
        out_specs=outs_at or [ON_CHIP] * len(outs),
        scratch_shapes=list(scratch),
        input_output_aliases=aliases or {},
        cost_estimate=pl.CostEstimate(
            flops=flops, bytes_accessed=nbytes, transcendentals=0
        ),
        compiler_params=pltpu.CompilerParams(vmem_limit_bytes=VMEM_LIMIT),
    )(*args)


def dot(a, b):
    return jnp.dot(a, b, preferred_element_type=jnp.float32)


def turned(v):
    half = v.shape[1] // 2
    return jnp.concatenate([-v[:, half:], v[:, :half]], axis=1)


def stacked(v):
    return jnp.concatenate([v, turned(v)], axis=0)


def both_sides(axis, count):
    here = lax.axis_index(axis)
    odd = lax.rem(here, 2)
    pair = here + 1 - 2 * odd
    other = lax.rem(here + count - 1 + 2 * odd, count)
    return here, pair, other


def span(list_ref, reader, owner, blocks):
    low = jnp.int32(blocks - 1)
    high = jnp.int32(0)
    for slot in range(list_ref.shape[0]):
        mine = list_ref[slot, 0, reader] == owner
        column = list_ref[slot, 2, reader]
        low = jnp.minimum(low, jnp.where(mine, column, low))
        high = jnp.maximum(high, jnp.where(mine, column, high))
    return low, high


def first_body(axis, count, *refs):
    x_hbm, leaf_hbm, self_hbm, cross_hbm, basis_hbm, tiles_hbm, list_hbm = refs[:7]
    coef_refs = refs[7 : 7 + CHUNKS]
    xb_ref, pair_ref, other_ref, self_ref, cross_ref, basis_ref, tiles_ref = refs[
        7 + CHUNKS : 14 + CHUNKS
    ]
    x_ref, leaf_ref, list_ref, sems = refs[14 + CHUNKS :]
    started = 0

    def fetch(source, target):
        nonlocal started
        copy = pltpu.make_async_copy(source, target, sems.at[started])
        started += 1
        copy.start()
        return copy

    def fetch_side_by_side(source, target):
        n = source.shape[-1]
        return [fetch(source.at[c], target.at[:, c * n : (c + 1) * n]) for c in range(2)]

    listing = fetch(list_hbm, list_ref)
    excitation = [fetch(x_hbm.at[c], x_ref.at[c]) for c in range(2)]
    leaf = fetch_side_by_side(leaf_hbm, leaf_ref)
    later = []
    for level in range(self_hbm.shape[0]):
        later += fetch_side_by_side(self_hbm.at[level], self_ref.at[level])
        later += fetch_side_by_side(cross_hbm.at[level], cross_ref.at[level])
    later += fetch_side_by_side(basis_hbm, basis_ref)
    later.append(fetch(tiles_hbm, tiles_ref))

    part = x_ref.shape[2] // CHUNKS
    for copy in excitation:
        copy.wait()
    for c in range(CHUNKS):
        for k in range(2):
            at = (2 * c + k) * part
            xb_ref[:, at : at + part] = x_ref[k, :, c * part : (c + 1) * part].astype(
                jnp.bfloat16
            )
    listing.wait()
    tile = pair_ref.shape[1]
    blocks = xb_ref.shape[0] // tile
    here, pair, other = both_sides(axis, count)
    for reader, ref in ((pair, pair_ref), (other, other_ref)):
        for k, column in enumerate(span(list_ref, reader, here, blocks)):
            rows = pl.ds(pl.multiple_of(column * tile, tile), tile)
            ref[k] = xb_ref[rows, :]
    for copy in leaf:
        copy.wait()
    for c, ref in enumerate(coef_refs):
        v = xb_ref[:, 2 * c * part : 2 * (c + 1) * part]
        ref[...] = dot(leaf_ref[...], stacked(v)).astype(ref.dtype)
    for copy in later:
        copy.wait()


def own_body(level, *refs):
    coef_refs, self_ref, out_refs = refs[:CHUNKS], refs[CHUNKS], refs[CHUNKS + 1 :]
    for coef_ref, out_ref in zip(coef_refs, out_refs):
        out_ref[...] = dot(self_ref[level], stacked(coef_ref[...]))


def cross_body(level, own_ref, partner_ref, cross_ref, out_ref):
    out_ref[...] = (
        own_ref[...] + dot(cross_ref[level], stacked(partner_ref[...]))
    ).astype(out_ref.dtype)


def near_body(axis, count, list_ref, tiles_ref, xb_ref, pair_ref, other_ref, near_ref, block_ref):
    tile = tiles_ref.shape[2]
    blocks = xb_ref.shape[0] // tile
    here, pair, other = both_sides(axis, count)
    pair_first, _ = span(list_ref, here, pair, blocks)
    other_first, _ = span(list_ref, here, other, blocks)
    near_ref[...] = jnp.zeros_like(near_ref)
    slots = tiles_ref.shape[0]
    for slot in range(slots):
        owner = list_ref[slot, 0, here]
        column = list_ref[slot, 2, here]

        @pl.when(owner == here)
        def _():
            rows = pl.ds(pl.multiple_of(column * tile, tile), tile)
            block_ref[slot] = xb_ref[rows, :]

        @pl.when(owner == pair)
        def _():
            block_ref[slot] = pair_ref[jnp.where(column == pair_first, 0, 1)]

        @pl.when(jnp.logical_and(owner == other, owner != pair))
        def _():
            block_ref[slot] = other_ref[jnp.where(column == other_first, 0, 1)]

        @pl.when(owner < 0)
        def _():
            block_ref[slot] = jnp.zeros(block_ref.shape[1:], block_ref.dtype)

    wide = 2 * xb_ref.shape[1] // (2 * CHUNKS)
    for slot in range(slots):
        row = list_ref[slot, 1, here]
        rows = pl.ds(pl.multiple_of(row * tile, tile), tile)
        for c in range(CHUNKS):
            v = block_ref[slot, :, c * wide : (c + 1) * wide]
            term = dot(tiles_ref[slot, 0], v) + dot(tiles_ref[slot, 1], turned(v))
            near_ref[rows, c * wide : (c + 1) * wide] += term


def last_body(level, c, *refs):
    own_ref, partner_ref, cross_ref, basis_ref, near_ref = refs[:5]
    out_hbm, result_ref, sems = refs[-3:]
    v = own_ref[...] + dot(cross_ref[level], stacked(partner_ref[...]))
    v = stacked(v.astype(jnp.bfloat16))
    part = v.shape[1] // 2
    rows = basis_ref.shape[0]
    step = rows // (sems.shape[0] // 2)
    copies = []
    for r in range(0, rows, step):
        result_ref[r : r + step, :] = (
            dot(basis_ref[r : r + step, :], v)
            + near_ref[r : r + step, 2 * c * part : 2 * (c + 1) * part]
        )
        for k in range(2):
            copy = pltpu.make_async_copy(
                result_ref.at[r : r + step, k * part : (k + 1) * part],
                out_hbm.at[k, r : r + step, c * part : (c + 1) * part],
                sems.at[len(copies)],
            )
            copy.start()
            copies.append(copy)
    for copy in copies:
        copy.wait()


def per_device(
    excitation, leaf_basis, self_transfer, cross_transfer, out_basis, near_tiles, near_list
):
    axis = "surf"
    count = lax.axis_size(axis)
    rows, width = excitation.shape[1:]
    rank = leaf_basis.shape[1]
    slots, _, tile, _ = near_tiles.shape
    levels = self_transfer.shape[0]
    part = width // CHUNKS
    bf16, f32 = jnp.bfloat16, jnp.float32
    listing = near_list.transpose(1, 2, 0)
    piece = pltpu.VMEM((rank, 2 * part), bf16)
    total = pltpu.VMEM((rank, 2 * part), f32)
    sent = pltpu.VMEM((2, tile, 2 * width), bf16)

    held = [
        pltpu.with_memory_space_constraint(a, pltpu.HBM)
        for a in (
            excitation,
            leaf_basis,
            self_transfer,
            cross_transfer,
            out_basis,
            near_tiles,
            listing,
        )
    ]
    first = call(
        functools.partial(first_body, axis, count),
        [piece] * CHUNKS
        + [
            pltpu.VMEM((rows, 2 * width), bf16),
            sent,
            sent,
            pltpu.VMEM((levels, rank, 2 * rank), bf16),
            pltpu.VMEM((levels, rank, 2 * rank), bf16),
            pltpu.VMEM((rows, 2 * rank), bf16),
            pltpu.VMEM(near_tiles.shape, bf16),
        ],
        [OFF_CHIP] * 7,
        held,
        8 * rank * rows * width,
        8 * rows * width,
        scratch=[
            pltpu.VMEM(excitation.shape, f32),
            pltpu.VMEM((rank, 2 * rows), bf16),
            pltpu.SMEM(listing.shape, jnp.int32),
            pltpu.SemaphoreType.DMA((8 + 4 * levels,)),
        ],
    )
    coef = first[:CHUNKS]
    xb, to_pair, to_other, self_maps, cross_maps, basis, tiles = first[CHUNKS:]
    for level in range(levels):
        swap = [(i, i ^ (1 << level)) for i in range(count)]
        partner = []
        for c in range(CHUNKS):
            partner.append(lax.ppermute(coef[c], axis, swap))
        if level == 1:
            to_pair, to_other, *coef = lax.optimization_barrier((to_pair, to_other, *coef))
            pair = lax.ppermute(to_pair, axis, [(i, i ^ 1) for i in range(count)])
            other = lax.ppermute(
                to_other, axis, [(i, (i + i % 2 * 2 - 1) % count) for i in range(count)]
            )
        own = call(
            functools.partial(own_body, level),
            [total] * CHUNKS,
            [ON_CHIP] * (CHUNKS + 1),
            (*coef, self_maps),
            8 * rank * rank * width,
            2 * rank * rank,
        )
        if level == levels - 1:
            break
        coef = []
        for c in range(CHUNKS):
            coef += call(
                functools.partial(cross_body, level),
                [piece],
                [ON_CHIP] * 3,
                (own[c], partner[c], cross_maps),
                8 * rank * rank * part,
                2 * rank * rank,
            )
    (near,) = call(
        functools.partial(near_body, axis, count),
        [pltpu.VMEM((rows, 2 * width), f32)],
        [SCALARS] + [ON_CHIP] * 4,
        (listing, tiles, xb, pair, other),
        8 * slots * tile * tile * width,
        8 * rows * width,
        scratch=[pltpu.VMEM((slots, tile, 2 * width), bf16)],
    )
    out = None
    for c in range(CHUNKS):
        before = () if out is None else (out,)
        (out,) = call(
            functools.partial(last_body, levels - 1, c),
            [jax.ShapeDtypeStruct((2, rows, width), f32)],
            [ON_CHIP] * 5 + [OFF_CHIP] * len(before),
            (own[c], partner[c], cross_maps, basis, near, *before),
            8 * rank * (rank + rows) * part,
            8 * rows * part,
            scratch=[pltpu.VMEM((rows, 2 * part), f32), pltpu.SemaphoreType.DMA((8,))],
            outs_at=[OFF_CHIP],
            aliases={5: 0} if before else {},
        )
    return out


def solution(mesh):
    placed = (
        P(None, "surf", None),
        P(None, "surf", None),
        P(None, None, "surf", None),
        P(None, None, "surf", None),
        P(None, "surf", None),
        P("surf", None, None, None),
        P(),
    )
    return jax.shard_map(
        per_device, mesh=mesh, in_specs=placed, out_specs=P(None, "surf", None), check_vma=False
    )
```

```python
import functools

import jax
import jax.numpy as jnp
from jax import lax
from jax.experimental import pallas as pl
from jax.experimental.pallas import tpu as pltpu
from jax.sharding import PartitionSpec as P


CHUNKS = 2
VMEM_LIMIT = 12 * 1024 * 1024
STEPS = 4

ON_CHIP = pl.BlockSpec(memory_space=pltpu.VMEM)
OFF_CHIP = pl.BlockSpec(memory_space=pltpu.HBM)
SCALARS = pl.BlockSpec(memory_space=pltpu.SMEM)


def call(body, outs, ins, args, flops, nbytes, scratch=(), outs_at=None, aliases=None):
    return pl.pallas_call(
        body,
        out_shape=outs,
        in_specs=ins,
        out_specs=outs_at or [ON_CHIP] * len(outs),
        scratch_shapes=list(scratch),
        input_output_aliases=aliases or {},
        cost_estimate=pl.CostEstimate(
            flops=flops, bytes_accessed=nbytes, transcendentals=0
        ),
        compiler_params=pltpu.CompilerParams(vmem_limit_bytes=VMEM_LIMIT),
    )(*args)


def dot(a, b):
    return jnp.dot(a, b, preferred_element_type=jnp.float32)


def turned(v):
    half = v.shape[1] // 2
    return jnp.concatenate([-v[:, half:], v[:, :half]], axis=1)


def stacked(*vs):
    return jnp.concatenate([w for v in vs for w in (v, turned(v))], axis=0)


def flat(ref, lanes):
    return jnp.concatenate([ref[k, :, lanes] for k in range(ref.shape[0])], axis=0)


def both_sides(axis, count):
    here = lax.axis_index(axis)
    odd = lax.rem(here, 2)
    pair = here + 1 - 2 * odd
    other = lax.rem(here + count - 1 + 2 * odd, count)
    return here, pair, other


def span(list_ref, reader, owner, blocks):
    low = jnp.int32(blocks - 1)
    high = jnp.int32(0)
    for slot in range(list_ref.shape[0]):
        mine = list_ref[slot, 0, reader] == owner
        column = list_ref[slot, 2, reader]
        low = jnp.minimum(low, jnp.where(mine, column, low))
        high = jnp.maximum(high, jnp.where(mine, column, high))
    return low, high


class Fetches:
    def __init__(self, sems):
        self.sems = sems
        self.count = 0

    def start(self, source, target):
        copy = pltpu.make_async_copy(source, target, self.sems.at[self.count])
        self.count += 1
        copy.start()
        return copy

    def side_by_side(self, source, target, at=0):
        n = source.shape[-1]
        return [
            self.start(source.at[c], target.at[:, at + c * n : at + (c + 1) * n])
            for c in range(2)
        ]

    def maps(self, level, self_hbm, cross_hbm, target):
        n = self_hbm.shape[-1]
        return self.side_by_side(self_hbm.at[level], target) + self.side_by_side(
            cross_hbm.at[level], target, 2 * n
        )


def first_body(axis, count, *refs):
    x_hbm, leaf_hbm, self_hbm, cross_hbm, list_hbm = refs[:5]
    coef_refs = refs[5 : 5 + CHUNKS]
    xb_ref, pair_ref, other_ref, *map_refs = refs[5 + CHUNKS : 10 + CHUNKS]
    x_ref, leaf_ref, list_ref, sems = refs[10 + CHUNKS :]
    fetches = Fetches(sems)
    listing = fetches.start(list_hbm, list_ref)
    excitation = [fetches.start(x_hbm.at[c], x_ref.at[c]) for c in range(2)]
    leaf = fetches.side_by_side(leaf_hbm, leaf_ref)
    later = []
    for level, ref in enumerate(map_refs):
        later += fetches.maps(level, self_hbm, cross_hbm, ref)

    part = x_ref.shape[2] // CHUNKS
    for copy in excitation:
        copy.wait()
    for c in range(CHUNKS):
        for k in range(2):
            at = (2 * c + k) * part
            xb_ref[:, at : at + part] = x_ref[k, :, c * part : (c + 1) * part].astype(
                jnp.bfloat16
            )
    listing.wait()
    tile = pair_ref.shape[1]
    blocks = xb_ref.shape[0] // tile
    here, pair, other = both_sides(axis, count)
    for reader, ref in ((pair, pair_ref), (other, other_ref)):
        for k, column in enumerate(span(list_ref, reader, here, blocks)):
            rows = pl.ds(pl.multiple_of(column * tile, tile), tile)
            ref[k] = xb_ref[rows, :]
    for copy in leaf:
        copy.wait()
    for c, ref in enumerate(coef_refs):
        v = xb_ref[:, 2 * c * part : 2 * (c + 1) * part]
        ref[...] = dot(leaf_ref[...], stacked(v)).astype(ref.dtype)
    for copy in later:
        copy.wait()


def rest_body(level, self_hbm, cross_hbm, basis_hbm, tiles_hbm, map_ref, basis_ref, tiles_ref, sems):
    fetches = Fetches(sems)
    copies = fetches.maps(level, self_hbm, cross_hbm, map_ref)
    copies += fetches.side_by_side(basis_hbm, basis_ref)
    copies.append(fetches.start(tiles_hbm, tiles_ref))
    for copy in copies:
        copy.wait()


def both_body(coef_ref, partner_ref, map_ref, out_ref):
    out_ref[...] = dot(map_ref[...], stacked(coef_ref[...], partner_ref[...])).astype(
        out_ref.dtype
    )


def own_body(*refs):
    coef_refs, map_ref, out_refs = refs[:CHUNKS], refs[CHUNKS], refs[CHUNKS + 1 :]
    half = map_ref.shape[1] // 2
    for coef_ref, out_ref in zip(coef_refs, out_refs):
        out_ref[...] = dot(map_ref[:, :half], stacked(coef_ref[...]))


def cross_body(own_ref, partner_ref, map_ref, out_ref):
    half = map_ref.shape[1] // 2
    out_ref[...] = (
        own_ref[...] + dot(map_ref[:, half:], stacked(partner_ref[...]))
    ).astype(out_ref.dtype)


def near_body(axis, count, list_ref, tiles_ref, xb_ref, pair_ref, near_ref, map_ref, block_ref):
    slots, _, tile, _ = tiles_ref.shape
    blocks = xb_ref.shape[0] // tile
    here, pair, other = both_sides(axis, count)
    pair_first, _ = span(list_ref, here, pair, blocks)
    other_first, _ = span(list_ref, here, other, blocks)
    near_ref[...] = jnp.zeros_like(near_ref)
    map_ref[...] = jnp.zeros_like(map_ref)
    half = map_ref.shape[1] // 2
    for slot in range(slots):
        owner = list_ref[slot, 0, here]
        column = list_ref[slot, 2, here]
        row = list_ref[slot, 1, here]

        @pl.when(owner == here)
        def _():
            rows = pl.ds(pl.multiple_of(column * tile, tile), tile)
            block_ref[slot] = xb_ref[rows, :]

        @pl.when(owner == pair)
        def _():
            block_ref[slot] = pair_ref[jnp.where(column == pair_first, 0, 1)]

        @pl.when(jnp.logical_and(owner != here, owner != pair))
        def _():
            block_ref[slot] = jnp.zeros(block_ref.shape[1:], block_ref.dtype)

        @pl.when(jnp.logical_and(owner == other, owner != pair))
        def _():
            rows = pl.ds(pl.multiple_of(row * tile, tile), tile)
            at = jnp.where(column == other_first, 0, tile)
            for k in range(2):
                cols = pl.ds(pl.multiple_of(at + k * half, tile), tile)
                map_ref[rows, cols] = (
                    map_ref[rows, cols].astype(jnp.float32)
                    + tiles_ref[slot, k].astype(jnp.float32)
                ).astype(map_ref.dtype)

    wide = xb_ref.shape[1] // CHUNKS
    for slot in range(slots):
        row = list_ref[slot, 1, here]
        rows = pl.ds(pl.multiple_of(row * tile, tile), tile)
        for c in range(CHUNKS):
            v = block_ref[slot, :, c * wide : (c + 1) * wide]
            term = dot(tiles_ref[slot, 0], v) + dot(tiles_ref[slot, 1], turned(v))
            near_ref[rows, c * wide : (c + 1) * wide] += term


def last_body(c, *refs):
    own_ref, partner_ref, map_ref, basis_ref, near_ref = refs[:5]
    if c == 0:
        side_ref, other_ref, out_hbm, sum_ref, result_ref, sems = refs[5:]
    else:
        _, out_hbm, result_ref, sems = refs[5:]
    half = map_ref.shape[1] // 2
    v = own_ref[...] + dot(map_ref[:, half:], stacked(partner_ref[...]))
    v = stacked(v.astype(jnp.bfloat16))
    wide = v.shape[1]
    part = wide // 2
    rows = basis_ref.shape[0]
    step = rows // STEPS
    copies = []
    if c == 0:
        side = [
            stacked(flat(other_ref, slice(d * wide, (d + 1) * wide))) for d in range(CHUNKS)
        ]
    for r in range(0, rows, step):
        piece = slice(r, r + step)
        total = dot(basis_ref[piece, :], v)
        if c == 0:
            total = total + near_ref[piece, :wide] + dot(side_ref[piece, :], side[0])
        else:
            total = total + near_ref[piece, (c - 1) * wide : c * wide]
        result_ref[piece, :] = total
        for k in range(2):
            copy = pltpu.make_async_copy(
                result_ref.at[piece, k * part : (k + 1) * part],
                out_hbm.at[k, piece, c * part : (c + 1) * part],
                sems.at[len(copies)],
            )
            copy.start()
            copies.append(copy)
    if c == 0:
        for d in range(1, CHUNKS):
            lanes = slice((d - 1) * wide, d * wide)
            sum_ref[:, lanes] = near_ref[:, d * wide : (d + 1) * wide] + dot(
                side_ref[...], side[d]
            )
    for copy in copies:
        copy.wait()


def per_device(
    excitation, leaf_basis, self_transfer, cross_transfer, out_basis, near_tiles, near_list
):
    axis = "surf"
    count = lax.axis_size(axis)
    rows, width = excitation.shape[1:]
    rank = leaf_basis.shape[1]
    slots, _, tile, _ = near_tiles.shape
    levels = self_transfer.shape[0]
    part = width // CHUNKS
    bf16, f32 = jnp.bfloat16, jnp.float32
    piece = pltpu.VMEM((rank, 2 * part), bf16)
    total = pltpu.VMEM((rank, 2 * part), f32)
    sent = pltpu.VMEM((2, tile, 2 * width), bf16)
    maps = pltpu.VMEM((rank, 4 * rank), bf16)
    pairs = [(i, i ^ 1) for i in range(count)]
    others = [(i, (i + i % 2 * 2 - 1) % count) for i in range(count)]

    def held(a):
        return pltpu.with_memory_space_constraint(a, pltpu.HBM)

    def swaps(level, coef):
        found = []
        for c in range(CHUNKS):
            found.append(lax.ppermute(coef[c], axis, [(i, i ^ (1 << level)) for i in range(count)]))
        return found

    self_transfer, cross_transfer = held(self_transfer), held(cross_transfer)
    listing = near_list.transpose(1, 2, 0)
    first = call(
        functools.partial(first_body, axis, count),
        [piece] * CHUNKS + [pltpu.VMEM((rows, 2 * width), bf16), sent, sent, maps, maps],
        [OFF_CHIP] * 5,
        (held(excitation), held(leaf_basis), self_transfer, cross_transfer, held(listing)),
        8 * rank * rows * width,
        8 * rows * width,
        scratch=[
            pltpu.VMEM(excitation.shape, f32),
            pltpu.VMEM((rank, 2 * rows), bf16),
            pltpu.SMEM(listing.shape, jnp.int32),
            pltpu.SemaphoreType.DMA((13,)),
        ],
    )
    coef = first[:CHUNKS]
    xb, to_pair, to_other, maps0, maps1 = first[CHUNKS:]

    partner = swaps(0, coef)
    pair = lax.ppermute(to_pair, axis, pairs)
    coef = [
        call(
            both_body,
            [piece],
            [ON_CHIP] * 3,
            (coef[c], partner[c], maps0),
            16 * rank * rank * part,
            4 * rank * rank,
        )[0]
        for c in range(CHUNKS)
    ]

    def own_products(level_maps, coef):
        return call(
            own_body,
            [total] * CHUNKS,
            [ON_CHIP] * (CHUNKS + 1),
            (*coef, level_maps),
            8 * rank * rank * width,
            2 * rank * rank,
        )

    partner = swaps(1, coef)
    own = own_products(maps1, coef)
    to_other, *own = lax.optimization_barrier((to_other, *own))
    other = lax.ppermute(to_other, axis, others)
    coef = [
        call(
            cross_body,
            [piece],
            [ON_CHIP] * 3,
            (own[c], partner[c], maps1),
            8 * rank * rank * part,
            2 * rank * rank,
        )[0]
        for c in range(CHUNKS)
    ]
    self_last, cross_last, out_basis, near_tiles, _ = lax.optimization_barrier(
        (self_transfer, cross_transfer, out_basis, near_tiles, coef[0])
    )
    maps2, basis, tiles = call(
        functools.partial(rest_body, levels - 1),
        [maps, pltpu.VMEM((rows, 2 * rank), bf16), pltpu.VMEM(near_tiles.shape, bf16)],
        [OFF_CHIP] * 4,
        (held(self_last), held(cross_last), held(out_basis), held(near_tiles)),
        8 * rank * rank * rank,
        8 * rank * rank,
        scratch=[pltpu.SemaphoreType.DMA((7,))],
    )
    partner = swaps(2, coef)
    own = own_products(maps2, coef)
    near, side = call(
        functools.partial(near_body, axis, count),
        [pltpu.VMEM((rows, 2 * width), f32), pltpu.VMEM((rows, 4 * tile), bf16)],
        [SCALARS] + [ON_CHIP] * 3,
        (listing, tiles, xb, pair),
        8 * slots * tile * tile * width,
        8 * rows * width,
        scratch=[pltpu.VMEM((slots, tile, 2 * width), bf16)],
    )
    out = sums = None
    for c in range(CHUNKS):
        outs = [jax.ShapeDtypeStruct((2, rows, width), f32)]
        if c == 0:
            extra, ins = (side, other), [ON_CHIP] * 2
            outs.append(pltpu.VMEM((rows, 2 * part * (CHUNKS - 1)), f32))
        else:
            near, extra, ins = sums, (out,), [OFF_CHIP]
        out, *left = call(
            functools.partial(last_body, c),
            outs,
            [ON_CHIP] * 5 + ins,
            (own[c], partner[c], maps2, basis, near, *extra),
            8 * rank * (rank + rows) * part,
            8 * rows * part,
            scratch=[
                pltpu.VMEM((rows, 2 * part), f32),
                pltpu.SemaphoreType.DMA((2 * STEPS,)),
            ],
            outs_at=[OFF_CHIP] + [ON_CHIP] * (len(outs) - 1),
            aliases={} if c == 0 else {5: 0},
        )
        sums = left[0] if left else sums
    return out


def solution(mesh):
    placed = (
        P(None, "surf", None),
        P(None, "surf", None),
        P(None, None, "surf", None),
        P(None, None, "surf", None),
        P(None, "surf", None),
        P("surf", None, None, None),
        P(),
    )
    return jax.shard_map(
        per_device, mesh=mesh, in_specs=placed, out_specs=P(None, "surf", None), check_vma=False
    )
```

```python
import functools

import jax
import jax.numpy as jnp
from jax import lax
from jax.experimental import pallas as pl
from jax.experimental.pallas import tpu as pltpu
from jax.sharding import PartitionSpec as P


CHUNKS = 2
VMEM_LIMIT = 12 * 1024 * 1024
STEPS = 4

ON_CHIP = pl.BlockSpec(memory_space=pltpu.VMEM)
OFF_CHIP = pl.BlockSpec(memory_space=pltpu.HBM)
SCALARS = pl.BlockSpec(memory_space=pltpu.SMEM)


def call(body, outs, ins, args, flops, nbytes, scratch=(), outs_at=None, aliases=None):
    return pl.pallas_call(
        body,
        out_shape=outs,
        in_specs=ins,
        out_specs=outs_at or [ON_CHIP] * len(outs),
        scratch_shapes=list(scratch),
        input_output_aliases=aliases or {},
        cost_estimate=pl.CostEstimate(
            flops=flops, bytes_accessed=nbytes, transcendentals=0
        ),
        compiler_params=pltpu.CompilerParams(vmem_limit_bytes=VMEM_LIMIT),
    )(*args)


def dot(a, b):
    return jnp.dot(a, b, preferred_element_type=jnp.float32)


def turned(v):
    half = v.shape[1] // 2
    return jnp.concatenate([-v[:, half:], v[:, :half]], axis=1)


def stacked(*vs):
    return jnp.concatenate([w for v in vs for w in (v, turned(v))], axis=0)


def chunk_lanes(width):
    step = 2 * width // CHUNKS
    return [slice(c * step, (c + 1) * step) for c in range(CHUNKS)]


def flat(ref, lanes):
    return jnp.concatenate([ref[k, :, lanes] for k in range(ref.shape[0])], axis=0)


def both_sides(axis, count):
    here = lax.axis_index(axis)
    odd = lax.rem(here, 2)
    pair = here + 1 - 2 * odd
    other = lax.rem(here + count - 1 + 2 * odd, count)
    return here, pair, other


def span(list_ref, reader, owner, blocks):
    low = jnp.int32(blocks - 1)
    high = jnp.int32(0)
    for slot in range(list_ref.shape[0]):
        mine = list_ref[slot, 0, reader] == owner
        column = list_ref[slot, 2, reader]
        low = jnp.minimum(low, jnp.where(mine, column, low))
        high = jnp.maximum(high, jnp.where(mine, column, high))
    return low, high


class Fetches:
    def __init__(self, sems):
        self.sems = sems
        self.count = 0

    def start(self, source, target):
        copy = pltpu.make_async_copy(source, target, self.sems.at[self.count])
        self.count += 1
        copy.start()
        return copy

    def side_by_side(self, source, target, at=0):
        n = source.shape[-1]
        return [
            self.start(source.at[c], target.at[:, at + c * n : at + (c + 1) * n])
            for c in range(2)
        ]

    def maps(self, level, self_hbm, cross_hbm, target):
        n = self_hbm.shape[-1]
        return self.side_by_side(self_hbm.at[level], target) + self.side_by_side(
            cross_hbm.at[level], target, 2 * n
        )


def first_body(axis, count, *refs):
    x_hbm, leaf_hbm, self_hbm, cross_hbm, list_hbm = refs[:5]
    coef_refs = refs[5 : 5 + CHUNKS]
    xb_ref, pair_ref, other_ref, *map_refs = refs[5 + CHUNKS : 10 + CHUNKS]
    x_ref, leaf_ref, list_ref, sems = refs[10 + CHUNKS :]
    fetches = Fetches(sems)
    listing = fetches.start(list_hbm, list_ref)
    excitation = [fetches.start(x_hbm.at[c], x_ref.at[c]) for c in range(2)]
    leaf = fetches.side_by_side(leaf_hbm, leaf_ref)
    later = []
    for level, ref in enumerate(map_refs):
        later += fetches.maps(level, self_hbm, cross_hbm, ref)

    width = x_ref.shape[2]
    half = width // CHUNKS
    for copy in excitation:
        copy.wait()
    for c in range(CHUNKS):
        for k in range(2):
            at = (2 * c + k) * half
            xb_ref[:, at : at + half] = x_ref[k, :, c * half : (c + 1) * half].astype(
                jnp.bfloat16
            )
    listing.wait()
    tile = pair_ref.shape[1]
    blocks = xb_ref.shape[0] // tile
    here, pair, other = both_sides(axis, count)
    for reader, ref in ((pair, pair_ref), (other, other_ref)):
        for k, column in enumerate(span(list_ref, reader, here, blocks)):
            rows = pl.ds(pl.multiple_of(column * tile, tile), tile)
            ref[k] = xb_ref[rows, :]
    for copy in leaf:
        copy.wait()
    for lanes, ref in zip(chunk_lanes(width), coef_refs):
        ref[...] = dot(leaf_ref[...], stacked(xb_ref[:, lanes])).astype(ref.dtype)
    for copy in later:
        copy.wait()


def rest_body(level, self_hbm, cross_hbm, basis_hbm, tiles_hbm, map_ref, basis_ref, tiles_ref, sems):
    fetches = Fetches(sems)
    copies = fetches.maps(level, self_hbm, cross_hbm, map_ref)
    copies += fetches.side_by_side(basis_hbm, basis_ref)
    copies.append(fetches.start(tiles_hbm, tiles_ref))
    for copy in copies:
        copy.wait()


def both_body(coef_ref, partner_ref, map_ref, out_ref):
    out_ref[...] = dot(map_ref[...], stacked(coef_ref[...], partner_ref[...])).astype(
        out_ref.dtype
    )


def own_body(*refs):
    coef_refs, map_ref, out_refs = refs[:CHUNKS], refs[CHUNKS], refs[CHUNKS + 1 :]
    half = map_ref.shape[1] // 2
    for coef_ref, out_ref in zip(coef_refs, out_refs):
        out_ref[...] = dot(map_ref[:, :half], stacked(coef_ref[...]))


def cross_body(own_ref, partner_ref, map_ref, out_ref):
    half = map_ref.shape[1] // 2
    out_ref[...] = (
        own_ref[...] + dot(map_ref[:, half:], stacked(partner_ref[...]))
    ).astype(out_ref.dtype)


def near_body(axis, count, list_ref, tiles_ref, xb_ref, pair_ref, near_ref, map_ref, block_ref):
    slots, _, tile, _ = tiles_ref.shape
    blocks = xb_ref.shape[0] // tile
    here, pair, other = both_sides(axis, count)
    pair_first, _ = span(list_ref, here, pair, blocks)
    other_first, _ = span(list_ref, here, other, blocks)
    near_ref[...] = jnp.zeros_like(near_ref)
    map_ref[...] = jnp.zeros_like(map_ref)
    half = map_ref.shape[1] // 2
    for slot in range(slots):
        owner = list_ref[slot, 0, here]
        column = list_ref[slot, 2, here]
        row = list_ref[slot, 1, here]

        @pl.when(owner == here)
        def _():
            rows = pl.ds(pl.multiple_of(column * tile, tile), tile)
            block_ref[slot] = xb_ref[rows, :]

        @pl.when(owner == pair)
        def _():
            block_ref[slot] = pair_ref[jnp.where(column == pair_first, 0, 1)]

        @pl.when(jnp.logical_and(owner != here, owner != pair))
        def _():
            block_ref[slot] = jnp.zeros(block_ref.shape[1:], block_ref.dtype)

        @pl.when(jnp.logical_and(owner == other, owner != pair))
        def _():
            rows = pl.ds(pl.multiple_of(row * tile, tile), tile)
            at = jnp.where(column == other_first, 0, tile)
            for k in range(2):
                cols = pl.ds(pl.multiple_of(at + k * half, tile), tile)
                map_ref[rows, cols] = (
                    map_ref[rows, cols].astype(jnp.float32)
                    + tiles_ref[slot, k].astype(jnp.float32)
                ).astype(map_ref.dtype)

    for slot in range(slots):
        row = list_ref[slot, 1, here]
        rows = pl.ds(pl.multiple_of(row * tile, tile), tile)
        for lanes in chunk_lanes(xb_ref.shape[1] // 2):
            v = block_ref[slot, :, lanes]
            term = dot(tiles_ref[slot, 0], v) + dot(tiles_ref[slot, 1], turned(v))
            near_ref[rows, lanes] += term


def base_body(*refs):
    coef_refs = refs[:CHUNKS]
    map_ref, basis_ref, near_ref, base_ref, fold_ref = refs[CHUNKS:]
    half = map_ref.shape[1] // 2
    for lanes, ref in zip(chunk_lanes(near_ref.shape[1] // 2), coef_refs):
        v = dot(map_ref[:, :half], stacked(ref[...])).astype(jnp.bfloat16)
        base_ref[:, lanes] = near_ref[:, lanes] + dot(basis_ref[...], stacked(v))
    fold_ref[...] = dot(basis_ref[...], stacked(map_ref[:, half:])).astype(fold_ref.dtype)


def send_rows(result_ref, out_hbm, sems, piece, at, number):
    half = result_ref.shape[1] // 2
    copies = []
    for k in range(2):
        copy = pltpu.make_async_copy(
            result_ref.at[piece, k * half : (k + 1) * half],
            out_hbm.at[k, piece, at : at + half],
            sems.at[2 * number + k],
        )
        copy.start()
        copies.append(copy)
    return copies


def last0_body(
    partner_ref, fold_ref, base_ref, side_ref, other_ref, out_hbm, left_ref, result_ref, sems
):
    rows, width = result_ref.shape
    main, small = chunk_lanes(width)
    v = stacked(partner_ref[...])
    near_main, near_small = stacked(flat(other_ref, main)), stacked(flat(other_ref, small))
    step = rows // STEPS
    copies = []
    for i in range(STEPS):
        piece = slice(i * step, (i + 1) * step)
        result_ref[piece, :] = (
            base_ref[piece, main]
            + dot(fold_ref[piece, :], v)
            + dot(side_ref[piece, :], near_main)
        )
        copies += send_rows(result_ref, out_hbm, sems, piece, 0, i)
    left_ref[...] = base_ref[:, small] + dot(side_ref[...], near_small)
    for copy in copies:
        copy.wait()


def last1_body(partner_ref, fold_ref, left_ref, before_hbm, out_hbm, result_ref, sems):
    rows, width = result_ref.shape
    v = stacked(partner_ref[...])
    step = rows // STEPS
    copies = []
    for i in range(STEPS):
        piece = slice(i * step, (i + 1) * step)
        result_ref[piece, :] = left_ref[piece, :] + dot(fold_ref[piece, :], v)
        copies += send_rows(result_ref, out_hbm, sems, piece, width // 2, i)
    for copy in copies:
        copy.wait()


def per_device(
    excitation, leaf_basis, self_transfer, cross_transfer, out_basis, near_tiles, near_list
):
    axis = "surf"
    count = lax.axis_size(axis)
    rows, width = excitation.shape[1:]
    rank = leaf_basis.shape[1]
    slots, _, tile, _ = near_tiles.shape
    levels = self_transfer.shape[0]
    bf16, f32 = jnp.bfloat16, jnp.float32
    sizes = [lanes.stop - lanes.start for lanes in chunk_lanes(width)]
    pieces = [pltpu.VMEM((rank, n), bf16) for n in sizes]
    totals = [pltpu.VMEM((rank, n), f32) for n in sizes]
    sent = pltpu.VMEM((2, tile, 2 * width), bf16)
    maps = pltpu.VMEM((rank, 4 * rank), bf16)
    pairs = [(i, i ^ 1) for i in range(count)]
    others = [(i, (i + i % 2 * 2 - 1) % count) for i in range(count)]

    def held(a):
        return pltpu.with_memory_space_constraint(a, pltpu.HBM)

    def swaps(level, coef):
        found = []
        for c in range(CHUNKS):
            found.append(lax.ppermute(coef[c], axis, [(i, i ^ (1 << level)) for i in range(count)]))
        return found

    self_transfer, cross_transfer = held(self_transfer), held(cross_transfer)
    listing = near_list.transpose(1, 2, 0)
    first = call(
        functools.partial(first_body, axis, count),
        pieces + [pltpu.VMEM((rows, 2 * width), bf16), sent, sent, maps, maps],
        [OFF_CHIP] * 5,
        (held(excitation), held(leaf_basis), self_transfer, cross_transfer, held(listing)),
        8 * rank * rows * width,
        8 * rows * width,
        scratch=[
            pltpu.VMEM(excitation.shape, f32),
            pltpu.VMEM((rank, 2 * rows), bf16),
            pltpu.SMEM(listing.shape, jnp.int32),
            pltpu.SemaphoreType.DMA((13,)),
        ],
    )
    coef = first[:CHUNKS]
    xb, to_pair, to_other, maps0, maps1 = first[CHUNKS:]

    partner = swaps(0, coef)
    pair = lax.ppermute(to_pair, axis, pairs)
    coef = [
        call(
            both_body,
            [pieces[c]],
            [ON_CHIP] * 3,
            (coef[c], partner[c], maps0),
            8 * rank * rank * sizes[c],
            4 * rank * rank,
        )[0]
        for c in range(CHUNKS)
    ]

    def own_products(level_maps, coef):
        return call(
            own_body,
            totals,
            [ON_CHIP] * (CHUNKS + 1),
            (*coef, level_maps),
            8 * rank * rank * width,
            2 * rank * rank,
        )

    partner = swaps(1, coef)
    own = own_products(maps1, coef)
    to_other, *own = lax.optimization_barrier((to_other, *own))
    other = lax.ppermute(to_other, axis, others)
    coef = [
        call(
            cross_body,
            [pieces[c]],
            [ON_CHIP] * 3,
            (own[c], partner[c], maps1),
            4 * rank * rank * sizes[c],
            2 * rank * rank,
        )[0]
        for c in range(CHUNKS)
    ]
    self_last, cross_last, out_basis, near_tiles, _ = lax.optimization_barrier(
        (self_transfer, cross_transfer, out_basis, near_tiles, own[0])
    )
    maps2, basis, tiles = call(
        functools.partial(rest_body, levels - 1),
        [maps, pltpu.VMEM((rows, 2 * rank), bf16), pltpu.VMEM(near_tiles.shape, bf16)],
        [OFF_CHIP] * 4,
        (held(self_last), held(cross_last), held(out_basis), held(near_tiles)),
        8 * rank * rank * rank,
        8 * rank * rank,
        scratch=[pltpu.SemaphoreType.DMA((7,))],
    )
    partner = swaps(2, coef)
    near, side = call(
        functools.partial(near_body, axis, count),
        [pltpu.VMEM((rows, 2 * width), f32), pltpu.VMEM((rows, 4 * tile), bf16)],
        [SCALARS] + [ON_CHIP] * 3,
        (listing, tiles, xb, pair),
        8 * slots * tile * tile * width,
        8 * rows * width,
        scratch=[pltpu.VMEM((slots, tile, 2 * width), bf16)],
    )
    base, fold = call(
        base_body,
        [pltpu.VMEM((rows, 2 * width), f32), pltpu.VMEM((rows, 2 * rank), bf16)],
        [ON_CHIP] * (CHUNKS + 3),
        (*coef, maps2, basis, near),
        8 * rows * rank * (rank + width),
        8 * rows * width,
    )
    whole = jax.ShapeDtypeStruct((2, rows, width), f32)
    scratch = [pltpu.VMEM((rows, width), f32), pltpu.SemaphoreType.DMA((2 * STEPS,))]
    out, left = call(
        last0_body,
        [whole, pltpu.VMEM((rows, width), f32)],
        [ON_CHIP] * 5,
        (partner[0], fold, base, side, other),
        8 * rows * (rank + tile) * width,
        8 * rows * width,
        scratch=scratch,
        outs_at=[OFF_CHIP, ON_CHIP],
    )
    return call(
        last1_body,
        [whole],
        [ON_CHIP] * 3 + [OFF_CHIP],
        (partner[1], fold, left, out),
        2 * rows * rank * width,
        4 * rows * width,
        scratch=scratch,
        outs_at=[OFF_CHIP],
        aliases={3: 0},
    )[0]


def solution(mesh):
    placed = (
        P(None, "surf", None),
        P(None, "surf", None),
        P(None, None, "surf", None),
        P(None, None, "surf", None),
        P(None, "surf", None),
        P("surf", None, None, None),
        P(),
    )
    return jax.shard_map(
        per_device, mesh=mesh, in_specs=placed, out_specs=P(None, "surf", None), check_vma=False
    )
```

```python
import functools

import jax
import jax.numpy as jnp
from jax import lax
from jax.experimental import pallas as pl
from jax.experimental.pallas import tpu as pltpu
from jax.sharding import PartitionSpec as P


CHUNKS = 2
VMEM_LIMIT = 12 * 1024 * 1024
STEPS = 4

ON_CHIP = pl.BlockSpec(memory_space=pltpu.VMEM)
OFF_CHIP = pl.BlockSpec(memory_space=pltpu.HBM)
SCALARS = pl.BlockSpec(memory_space=pltpu.SMEM)


def call(body, outs, ins, args, flops, nbytes, scratch=(), outs_at=None, aliases=None):
    return pl.pallas_call(
        body,
        out_shape=outs,
        in_specs=ins,
        out_specs=outs_at or [ON_CHIP] * len(outs),
        scratch_shapes=list(scratch),
        input_output_aliases=aliases or {},
        cost_estimate=pl.CostEstimate(
            flops=flops, bytes_accessed=nbytes, transcendentals=0
        ),
        compiler_params=pltpu.CompilerParams(vmem_limit_bytes=VMEM_LIMIT),
    )(*args)


def dot(a, b):
    return jnp.dot(a, b, preferred_element_type=jnp.float32)


def turned(v):
    half = v.shape[1] // 2
    return jnp.concatenate([-v[:, half:], v[:, :half]], axis=1)


def stacked(*vs):
    return jnp.concatenate([w for v in vs for w in (v, turned(v))], axis=0)


def chunk_lanes(width):
    step = 2 * width // CHUNKS
    return [slice(c * step, (c + 1) * step) for c in range(CHUNKS)]


def flat(ref, lanes):
    return jnp.concatenate([ref[k, :, lanes] for k in range(ref.shape[0])], axis=0)


def both_sides(axis, count):
    here = lax.axis_index(axis)
    odd = lax.rem(here, 2)
    pair = here + 1 - 2 * odd
    other = lax.rem(here + count - 1 + 2 * odd, count)
    return here, pair, other


def span(list_ref, reader, owner, blocks):
    low = jnp.int32(blocks - 1)
    high = jnp.int32(0)
    for slot in range(list_ref.shape[0]):
        mine = list_ref[slot, 0, reader] == owner
        column = list_ref[slot, 2, reader]
        low = jnp.minimum(low, jnp.where(mine, column, low))
        high = jnp.maximum(high, jnp.where(mine, column, high))
    return low, high


class Fetches:
    def __init__(self, sems):
        self.sems = sems
        self.count = 0

    def start(self, source, target):
        copy = pltpu.make_async_copy(source, target, self.sems.at[self.count])
        self.count += 1
        copy.start()
        return copy

    def side_by_side(self, source, target, at=0):
        n = source.shape[-1]
        return [
            self.start(source.at[c], target.at[:, at + c * n : at + (c + 1) * n])
            for c in range(2)
        ]

    def maps(self, level, self_hbm, cross_hbm, target):
        n = self_hbm.shape[-1]
        return self.side_by_side(self_hbm.at[level], target) + self.side_by_side(
            cross_hbm.at[level], target, 2 * n
        )


def first_body(axis, count, *refs):
    x_hbm, leaf_hbm, self_hbm, cross_hbm, list_hbm = refs[:5]
    coef_refs = refs[5 : 5 + CHUNKS]
    xb_ref, pair_ref, other_ref, *map_refs = refs[5 + CHUNKS : 10 + CHUNKS]
    x_ref, leaf_ref, list_ref, sems = refs[10 + CHUNKS :]
    fetches = Fetches(sems)
    listing = fetches.start(list_hbm, list_ref)
    excitation = [fetches.start(x_hbm.at[c], x_ref.at[c]) for c in range(2)]
    leaf = fetches.side_by_side(leaf_hbm, leaf_ref)
    later = []
    for level, ref in enumerate(map_refs):
        later += fetches.maps(level, self_hbm, cross_hbm, ref)

    width = x_ref.shape[2]
    half = width // CHUNKS
    for copy in excitation:
        copy.wait()
    for c in range(CHUNKS):
        for k in range(2):
            at = (2 * c + k) * half
            xb_ref[:, at : at + half] = x_ref[k, :, c * half : (c + 1) * half].astype(
                jnp.bfloat16
            )
    listing.wait()
    tile = pair_ref.shape[1]
    blocks = xb_ref.shape[0] // tile
    here, pair, other = both_sides(axis, count)
    for reader, ref in ((pair, pair_ref), (other, other_ref)):
        for k, column in enumerate(span(list_ref, reader, here, blocks)):
            rows = pl.ds(pl.multiple_of(column * tile, tile), tile)
            ref[k] = xb_ref[rows, :]
    for copy in leaf:
        copy.wait()
    for lanes, ref in zip(chunk_lanes(width), coef_refs):
        ref[...] = dot(leaf_ref[...], stacked(xb_ref[:, lanes])).astype(ref.dtype)
    for copy in later:
        copy.wait()


def rest_body(axis, turn, level, *refs):
    self_hbm, cross_hbm, basis_hbm, tiles_hbm = refs[:4]
    map_ref, basis_ref, tiles_ref, sems = refs[-4:]
    here = lax.axis_index(axis)
    early = jnp.logical_and(lax.rem(here, 2) == 0, here > 0)

    @pl.when(early if turn == 0 else jnp.logical_not(early))
    def _():
        fetches = Fetches(sems)
        copies = fetches.maps(level, self_hbm, cross_hbm, map_ref)
        copies += fetches.side_by_side(basis_hbm, basis_ref)
        copies.append(fetches.start(tiles_hbm, tiles_ref))
        for copy in copies:
            copy.wait()


def own_body(*refs):
    coef_refs, map_ref, out_refs = refs[:CHUNKS], refs[CHUNKS], refs[CHUNKS + 1 :]
    half = map_ref.shape[1] // 2
    for coef_ref, out_ref in zip(coef_refs, out_refs):
        out_ref[...] = dot(map_ref[:, :half], stacked(coef_ref[...]))


def cross_body(own_ref, partner_ref, map_ref, out_ref):
    half = map_ref.shape[1] // 2
    out_ref[...] = (
        own_ref[...] + dot(map_ref[:, half:], stacked(partner_ref[...]))
    ).astype(out_ref.dtype)


def near_body(axis, count, list_ref, tiles_ref, xb_ref, pair_ref, near_ref, map_ref, block_ref):
    slots, _, tile, _ = tiles_ref.shape
    blocks = xb_ref.shape[0] // tile
    here, pair, other = both_sides(axis, count)
    pair_first, _ = span(list_ref, here, pair, blocks)
    other_first, _ = span(list_ref, here, other, blocks)
    near_ref[...] = jnp.zeros_like(near_ref)
    map_ref[...] = jnp.zeros_like(map_ref)
    half = map_ref.shape[1] // 2
    for slot in range(slots):
        owner = list_ref[slot, 0, here]
        column = list_ref[slot, 2, here]
        row = list_ref[slot, 1, here]

        @pl.when(owner == here)
        def _():
            rows = pl.ds(pl.multiple_of(column * tile, tile), tile)
            block_ref[slot] = xb_ref[rows, :]

        @pl.when(owner == pair)
        def _():
            block_ref[slot] = pair_ref[jnp.where(column == pair_first, 0, 1)]

        @pl.when(jnp.logical_and(owner != here, owner != pair))
        def _():
            block_ref[slot] = jnp.zeros(block_ref.shape[1:], block_ref.dtype)

        @pl.when(jnp.logical_and(owner == other, owner != pair))
        def _():
            rows = pl.ds(pl.multiple_of(row * tile, tile), tile)
            at = jnp.where(column == other_first, 0, tile)
            for k in range(2):
                cols = pl.ds(pl.multiple_of(at + k * half, tile), tile)
                map_ref[rows, cols] = (
                    map_ref[rows, cols].astype(jnp.float32)
                    + tiles_ref[slot, k].astype(jnp.float32)
                ).astype(map_ref.dtype)

    for slot in range(slots):
        row = list_ref[slot, 1, here]
        rows = pl.ds(pl.multiple_of(row * tile, tile), tile)
        for lanes in chunk_lanes(xb_ref.shape[1] // 2):
            v = block_ref[slot, :, lanes]
            term = dot(tiles_ref[slot, 0], v) + dot(tiles_ref[slot, 1], turned(v))
            near_ref[rows, lanes] += term


def base_body(*refs):
    coef_refs = refs[:CHUNKS]
    map_ref, basis_ref, near_ref, base_ref, fold_ref = refs[CHUNKS:]
    half = map_ref.shape[1] // 2
    for lanes, ref in zip(chunk_lanes(near_ref.shape[1] // 2), coef_refs):
        v = dot(map_ref[:, :half], stacked(ref[...])).astype(jnp.bfloat16)
        base_ref[:, lanes] = near_ref[:, lanes] + dot(basis_ref[...], stacked(v))
    fold_ref[...] = dot(basis_ref[...], stacked(map_ref[:, half:])).astype(fold_ref.dtype)


def send_rows(result_ref, out_hbm, sems, piece, at, number):
    half = result_ref.shape[1] // 2
    copies = []
    for k in range(2):
        copy = pltpu.make_async_copy(
            result_ref.at[piece, k * half : (k + 1) * half],
            out_hbm.at[k, piece, at : at + half],
            sems.at[2 * number + k],
        )
        copy.start()
        copies.append(copy)
    return copies


def last0_body(
    partner_ref, fold_ref, base_ref, side_ref, other_ref, out_hbm, left_ref, result_ref, sems
):
    rows, width = result_ref.shape
    main, small = chunk_lanes(width)
    v = stacked(partner_ref[...])
    near_main, near_small = stacked(flat(other_ref, main)), stacked(flat(other_ref, small))
    step = rows // STEPS
    copies = []
    for i in range(STEPS):
        piece = slice(i * step, (i + 1) * step)
        result_ref[piece, :] = (
            base_ref[piece, main]
            + dot(fold_ref[piece, :], v)
            + dot(side_ref[piece, :], near_main)
        )
        copies += send_rows(result_ref, out_hbm, sems, piece, 0, i)
    left_ref[...] = base_ref[:, small] + dot(side_ref[...], near_small)
    for copy in copies:
        copy.wait()


def last1_body(partner_ref, fold_ref, left_ref, before_hbm, out_hbm, result_ref, sems):
    rows, width = result_ref.shape
    v = stacked(partner_ref[...])
    step = rows // STEPS
    copies = []
    for i in range(STEPS):
        piece = slice(i * step, (i + 1) * step)
        result_ref[piece, :] = left_ref[piece, :] + dot(fold_ref[piece, :], v)
        copies += send_rows(result_ref, out_hbm, sems, piece, width // 2, i)
    for copy in copies:
        copy.wait()


def per_device(
    excitation, leaf_basis, self_transfer, cross_transfer, out_basis, near_tiles, near_list
):
    axis = "surf"
    count = lax.axis_size(axis)
    rows, width = excitation.shape[1:]
    rank = leaf_basis.shape[1]
    slots, _, tile, _ = near_tiles.shape
    levels = self_transfer.shape[0]
    bf16, f32 = jnp.bfloat16, jnp.float32
    sizes = [lanes.stop - lanes.start for lanes in chunk_lanes(width)]
    pieces = [pltpu.VMEM((rank, n), bf16) for n in sizes]
    totals = [pltpu.VMEM((rank, n), f32) for n in sizes]
    sent = pltpu.VMEM((2, tile, 2 * width), bf16)
    maps = pltpu.VMEM((rank, 4 * rank), bf16)
    pairs = [(i, i ^ 1) for i in range(count)]
    others = [(i, (i + i % 2 * 2 - 1) % count) for i in range(count)]

    def held(a):
        return pltpu.with_memory_space_constraint(a, pltpu.HBM)

    def swaps(level, coef):
        found = []
        for c in range(CHUNKS):
            found.append(lax.ppermute(coef[c], axis, [(i, i ^ (1 << level)) for i in range(count)]))
        return found

    def own_products(level_maps, coef):
        return call(
            own_body,
            totals,
            [ON_CHIP] * (CHUNKS + 1),
            (*coef, level_maps),
            8 * rank * rank * width,
            2 * rank * rank,
        )

    def rest(turn, after, before=()):
        late = lax.optimization_barrier(
            (self_transfer, cross_transfer, out_basis, near_tiles, after)
        )
        return call(
            functools.partial(rest_body, axis, turn, levels - 1),
            [maps, pltpu.VMEM((rows, 2 * rank), bf16), pltpu.VMEM(near_tiles.shape, bf16)],
            [OFF_CHIP] * 4 + [ON_CHIP] * len(before),
            (*[held(a) for a in late[:4]], *before),
            8 * rank * rank * rank,
            8 * rank * rank,
            scratch=[pltpu.SemaphoreType.DMA((7,))],
            aliases={4 + k: k for k in range(len(before))},
        )

    self_transfer, cross_transfer = held(self_transfer), held(cross_transfer)
    listing = near_list.transpose(1, 2, 0)
    first = call(
        functools.partial(first_body, axis, count),
        pieces + [pltpu.VMEM((rows, 2 * width), bf16), sent, sent, maps, maps],
        [OFF_CHIP] * 5,
        (held(excitation), held(leaf_basis), self_transfer, cross_transfer, held(listing)),
        8 * rank * rows * width,
        8 * rows * width,
        scratch=[
            pltpu.VMEM(excitation.shape, f32),
            pltpu.VMEM((rank, 2 * rows), bf16),
            pltpu.SMEM(listing.shape, jnp.int32),
            pltpu.SemaphoreType.DMA((13,)),
        ],
    )
    coef = first[:CHUNKS]
    xb, to_pair, to_other, maps0, maps1 = first[CHUNKS:]

    partner = swaps(0, coef)
    pair = lax.ppermute(to_pair, axis, pairs)
    own = own_products(maps0, coef)
    coef = [
        call(
            cross_body,
            [pieces[c]],
            [ON_CHIP] * 3,
            (own[c], partner[c], maps0),
            8 * rank * rank * sizes[c],
            4 * rank * rank,
        )[0]
        for c in range(CHUNKS)
    ]

    partner = swaps(1, coef)
    own = own_products(maps1, coef)
    to_other, *own = lax.optimization_barrier((to_other, *own))
    other = lax.ppermute(to_other, axis, others)
    coef = [
        call(
            cross_body,
            [pieces[c]],
            [ON_CHIP] * 3,
            (own[c], partner[c], maps1),
            4 * rank * rank * sizes[c],
            2 * rank * rank,
        )[0]
        for c in range(CHUNKS)
    ]
    maps2, basis, tiles = rest(1, coef[0], rest(0, own[0]))
    partner = swaps(2, coef)
    near, side = call(
        functools.partial(near_body, axis, count),
        [pltpu.VMEM((rows, 2 * width), f32), pltpu.VMEM((rows, 4 * tile), bf16)],
        [SCALARS] + [ON_CHIP] * 3,
        (listing, tiles, xb, pair),
        8 * slots * tile * tile * width,
        8 * rows * width,
        scratch=[pltpu.VMEM((slots, tile, 2 * width), bf16)],
    )
    base, fold = call(
        base_body,
        [pltpu.VMEM((rows, 2 * width), f32), pltpu.VMEM((rows, 2 * rank), bf16)],
        [ON_CHIP] * (CHUNKS + 3),
        (*coef, maps2, basis, near),
        8 * rows * rank * (rank + width),
        8 * rows * width,
    )
    whole = jax.ShapeDtypeStruct((2, rows, width), f32)
    scratch = [pltpu.VMEM((rows, width), f32), pltpu.SemaphoreType.DMA((2 * STEPS,))]
    out, left = call(
        last0_body,
        [whole, pltpu.VMEM((rows, width), f32)],
        [ON_CHIP] * 5,
        (partner[0], fold, base, side, other),
        8 * rows * (rank + tile) * width,
        8 * rows * width,
        scratch=scratch,
        outs_at=[OFF_CHIP, ON_CHIP],
    )
    return call(
        last1_body,
        [whole],
        [ON_CHIP] * 3 + [OFF_CHIP],
        (partner[1], fold, left, out),
        2 * rows * rank * width,
        4 * rows * width,
        scratch=scratch,
        outs_at=[OFF_CHIP],
        aliases={3: 0},
    )[0]


def solution(mesh):
    placed = (
        P(None, "surf", None),
        P(None, "surf", None),
        P(None, None, "surf", None),
        P(None, None, "surf", None),
        P(None, "surf", None),
        P("surf", None, None, None),
        P(),
    )
    return jax.shard_map(
        per_device, mesh=mesh, in_specs=placed, out_specs=P(None, "surf", None), check_vma=False
    )
```

```python
import functools

import jax
import jax.numpy as jnp
from jax import lax
from jax.experimental import pallas as pl
from jax.experimental.pallas import tpu as pltpu
from jax.sharding import PartitionSpec as P


CHUNKS = 2
VMEM_LIMIT = 12 * 1024 * 1024
STEPS = 4

ON_CHIP = pl.BlockSpec(memory_space=pltpu.VMEM)
OFF_CHIP = pl.BlockSpec(memory_space=pltpu.HBM)
SCALARS = pl.BlockSpec(memory_space=pltpu.SMEM)


def call(body, outs, ins, args, flops, nbytes, scratch=(), outs_at=None, aliases=None):
    return pl.pallas_call(
        body,
        out_shape=outs,
        in_specs=ins,
        out_specs=outs_at or [ON_CHIP] * len(outs),
        scratch_shapes=list(scratch),
        input_output_aliases=aliases or {},
        cost_estimate=pl.CostEstimate(
            flops=flops, bytes_accessed=nbytes, transcendentals=0
        ),
        compiler_params=pltpu.CompilerParams(vmem_limit_bytes=VMEM_LIMIT),
    )(*args)


def dot(a, b):
    return jnp.dot(a, b, preferred_element_type=jnp.float32)


def turned(v):
    half = v.shape[1] // 2
    return jnp.concatenate([-v[:, half:], v[:, :half]], axis=1)


def stacked(*vs):
    return jnp.concatenate([w for v in vs for w in (v, turned(v))], axis=0)


def chunk_lanes(width):
    step = 2 * width // CHUNKS
    return [slice(c * step, (c + 1) * step) for c in range(CHUNKS)]


def flat(ref, lanes):
    return jnp.concatenate([ref[k, :, lanes] for k in range(ref.shape[0])], axis=0)


def both_sides(axis, count):
    here = lax.axis_index(axis)
    odd = lax.rem(here, 2)
    pair = here + 1 - 2 * odd
    other = lax.rem(here + count - 1 + 2 * odd, count)
    return here, pair, other


def span(list_ref, reader, owner, blocks):
    low = jnp.int32(blocks - 1)
    high = jnp.int32(0)
    for slot in range(list_ref.shape[0]):
        mine = list_ref[slot, 0, reader] == owner
        column = list_ref[slot, 2, reader]
        low = jnp.minimum(low, jnp.where(mine, column, low))
        high = jnp.maximum(high, jnp.where(mine, column, high))
    return low, high


class Fetches:
    def __init__(self, sems):
        self.sems = sems
        self.count = 0

    def start(self, source, target):
        copy = pltpu.make_async_copy(source, target, self.sems.at[self.count])
        self.count += 1
        copy.start()
        return copy

    def side_by_side(self, source, target, at=0):
        n = source.shape[-1]
        return [
            self.start(source.at[c], target.at[:, at + c * n : at + (c + 1) * n])
            for c in range(2)
        ]

    def maps(self, level, self_hbm, cross_hbm, target):
        n = self_hbm.shape[-1]
        return self.side_by_side(self_hbm.at[level], target) + self.side_by_side(
            cross_hbm.at[level], target, 2 * n
        )


def first_body(axis, count, *refs):
    x_hbm, leaf_hbm, self_hbm, cross_hbm, list_hbm = refs[:5]
    coef_refs = refs[5 : 5 + CHUNKS]
    xb_ref, pair_ref, other_ref, *map_refs = refs[5 + CHUNKS : 10 + CHUNKS]
    x_ref, leaf_ref, list_ref, sems = refs[10 + CHUNKS :]
    fetches = Fetches(sems)
    listing = fetches.start(list_hbm, list_ref)
    excitation = [fetches.start(x_hbm.at[c], x_ref.at[c]) for c in range(2)]
    leaf = fetches.side_by_side(leaf_hbm, leaf_ref)
    later = []
    for level, ref in enumerate(map_refs):
        later += fetches.maps(level, self_hbm, cross_hbm, ref)

    width = x_ref.shape[2]
    half = width // CHUNKS
    for copy in excitation:
        copy.wait()
    for c in range(CHUNKS):
        for k in range(2):
            at = (2 * c + k) * half
            xb_ref[:, at : at + half] = x_ref[k, :, c * half : (c + 1) * half].astype(
                jnp.bfloat16
            )
    listing.wait()
    tile = pair_ref.shape[1]
    blocks = xb_ref.shape[0] // tile
    here, pair, other = both_sides(axis, count)
    for reader, ref in ((pair, pair_ref), (other, other_ref)):
        for k, column in enumerate(span(list_ref, reader, here, blocks)):
            rows = pl.ds(pl.multiple_of(column * tile, tile), tile)
            ref[k] = xb_ref[rows, :]
    for copy in leaf:
        copy.wait()
    for lanes, ref in zip(chunk_lanes(width), coef_refs):
        ref[...] = dot(leaf_ref[...], stacked(xb_ref[:, lanes])).astype(ref.dtype)
    for copy in later:
        copy.wait()


def rest_body(axis, turn, level, *refs):
    self_hbm, cross_hbm, basis_hbm, tiles_hbm = refs[:4]
    map_ref, basis_ref, tiles_ref, sems = refs[-4:]
    here = lax.axis_index(axis)
    early = jnp.logical_and(lax.rem(here, 2) == 0, here > 0)

    fetches = Fetches(sems)

    @pl.when(early if turn == 0 else jnp.logical_not(early))
    def _():
        for copy in fetches.maps(level, self_hbm, cross_hbm, map_ref):
            copy.wait()

    if turn:
        copies = fetches.side_by_side(basis_hbm, basis_ref)
        copies.append(fetches.start(tiles_hbm, tiles_ref))
        for copy in copies:
            copy.wait()


def own_body(*refs):
    coef_refs, map_ref, out_refs = refs[:CHUNKS], refs[CHUNKS], refs[CHUNKS + 1 :]
    half = map_ref.shape[1] // 2
    for coef_ref, out_ref in zip(coef_refs, out_refs):
        out_ref[...] = dot(map_ref[:, :half], stacked(coef_ref[...]))


def cross_body(own_ref, partner_ref, map_ref, out_ref):
    half = map_ref.shape[1] // 2
    out_ref[...] = (
        own_ref[...] + dot(map_ref[:, half:], stacked(partner_ref[...]))
    ).astype(out_ref.dtype)


def near_body(axis, count, list_ref, tiles_ref, xb_ref, pair_ref, near_ref, map_ref, block_ref):
    slots, _, tile, _ = tiles_ref.shape
    blocks = xb_ref.shape[0] // tile
    here, pair, other = both_sides(axis, count)
    pair_first, _ = span(list_ref, here, pair, blocks)
    other_first, _ = span(list_ref, here, other, blocks)
    near_ref[...] = jnp.zeros_like(near_ref)
    map_ref[...] = jnp.zeros_like(map_ref)
    half = map_ref.shape[1] // 2
    for slot in range(slots):
        owner = list_ref[slot, 0, here]
        column = list_ref[slot, 2, here]
        row = list_ref[slot, 1, here]

        @pl.when(owner == here)
        def _():
            rows = pl.ds(pl.multiple_of(column * tile, tile), tile)
            block_ref[slot] = xb_ref[rows, :]

        @pl.when(owner == pair)
        def _():
            block_ref[slot] = pair_ref[jnp.where(column == pair_first, 0, 1)]

        @pl.when(jnp.logical_and(owner != here, owner != pair))
        def _():
            block_ref[slot] = jnp.zeros(block_ref.shape[1:], block_ref.dtype)

        @pl.when(jnp.logical_and(owner == other, owner != pair))
        def _():
            rows = pl.ds(pl.multiple_of(row * tile, tile), tile)
            at = jnp.where(column == other_first, 0, tile)
            for k in range(2):
                cols = pl.ds(pl.multiple_of(at + k * half, tile), tile)
                map_ref[rows, cols] = (
                    map_ref[rows, cols].astype(jnp.float32)
                    + tiles_ref[slot, k].astype(jnp.float32)
                ).astype(map_ref.dtype)

    for slot in range(slots):
        row = list_ref[slot, 1, here]
        rows = pl.ds(pl.multiple_of(row * tile, tile), tile)
        for lanes in chunk_lanes(xb_ref.shape[1] // 2):
            v = block_ref[slot, :, lanes]
            term = dot(tiles_ref[slot, 0], v) + dot(tiles_ref[slot, 1], turned(v))
            near_ref[rows, lanes] += term


def base_body(*refs):
    coef_refs = refs[:CHUNKS]
    map_ref, basis_ref, near_ref, base_ref, fold_ref = refs[CHUNKS:]
    half = map_ref.shape[1] // 2
    for lanes, ref in zip(chunk_lanes(near_ref.shape[1] // 2), coef_refs):
        v = dot(map_ref[:, :half], stacked(ref[...])).astype(jnp.bfloat16)
        base_ref[:, lanes] = near_ref[:, lanes] + dot(basis_ref[...], stacked(v))
    fold_ref[...] = dot(basis_ref[...], stacked(map_ref[:, half:])).astype(fold_ref.dtype)


def send_rows(result_ref, out_hbm, sems, piece, at, number):
    half = result_ref.shape[1] // 2
    copies = []
    for k in range(2):
        copy = pltpu.make_async_copy(
            result_ref.at[piece, k * half : (k + 1) * half],
            out_hbm.at[k, piece, at : at + half],
            sems.at[2 * number + k],
        )
        copy.start()
        copies.append(copy)
    return copies


def last0_body(
    partner_ref, fold_ref, base_ref, side_ref, other_ref, out_hbm, left_ref, result_ref, sems
):
    rows, width = result_ref.shape
    main, small = chunk_lanes(width)
    v = stacked(partner_ref[...])
    near_main, near_small = stacked(flat(other_ref, main)), stacked(flat(other_ref, small))
    step = rows // STEPS
    copies = []
    for i in range(STEPS):
        piece = slice(i * step, (i + 1) * step)
        result_ref[piece, :] = (
            base_ref[piece, main]
            + dot(fold_ref[piece, :], v)
            + dot(side_ref[piece, :], near_main)
        )
        copies += send_rows(result_ref, out_hbm, sems, piece, 0, i)
    left_ref[...] = base_ref[:, small] + dot(side_ref[...], near_small)
    for copy in copies:
        copy.wait()


def last1_body(partner_ref, fold_ref, left_ref, before_hbm, out_hbm, result_ref, sems):
    rows, width = result_ref.shape
    v = stacked(partner_ref[...])
    step = rows // STEPS
    copies = []
    for i in range(STEPS):
        piece = slice(i * step, (i + 1) * step)
        result_ref[piece, :] = left_ref[piece, :] + dot(fold_ref[piece, :], v)
        copies += send_rows(result_ref, out_hbm, sems, piece, width // 2, i)
    for copy in copies:
        copy.wait()


def per_device(
    excitation, leaf_basis, self_transfer, cross_transfer, out_basis, near_tiles, near_list
):
    axis = "surf"
    count = lax.axis_size(axis)
    rows, width = excitation.shape[1:]
    rank = leaf_basis.shape[1]
    slots, _, tile, _ = near_tiles.shape
    levels = self_transfer.shape[0]
    bf16, f32 = jnp.bfloat16, jnp.float32
    sizes = [lanes.stop - lanes.start for lanes in chunk_lanes(width)]
    pieces = [pltpu.VMEM((rank, n), bf16) for n in sizes]
    totals = [pltpu.VMEM((rank, n), f32) for n in sizes]
    sent = pltpu.VMEM((2, tile, 2 * width), bf16)
    maps = pltpu.VMEM((rank, 4 * rank), bf16)
    pairs = [(i, i ^ 1) for i in range(count)]
    others = [(i, (i + i % 2 * 2 - 1) % count) for i in range(count)]

    def held(a):
        return pltpu.with_memory_space_constraint(a, pltpu.HBM)

    def swaps(level, coef):
        found = []
        for c in range(CHUNKS):
            found.append(lax.ppermute(coef[c], axis, [(i, i ^ (1 << level)) for i in range(count)]))
        return found

    def own_products(level_maps, coef):
        return call(
            own_body,
            totals,
            [ON_CHIP] * (CHUNKS + 1),
            (*coef, level_maps),
            8 * rank * rank * width,
            2 * rank * rank,
        )

    def rest(turn, after, before=()):
        late = lax.optimization_barrier(
            (self_transfer, cross_transfer, out_basis, near_tiles, after)
        )
        return call(
            functools.partial(rest_body, axis, turn, levels - 1),
            [maps, pltpu.VMEM((rows, 2 * rank), bf16), pltpu.VMEM(near_tiles.shape, bf16)],
            [OFF_CHIP] * 4 + [ON_CHIP] * len(before),
            (*[held(a) for a in late[:4]], *before),
            8 * rank * rank * rank,
            8 * rank * rank,
            scratch=[pltpu.SemaphoreType.DMA((7,))],
            aliases={4 + k: k for k in range(len(before))},
        )

    self_transfer, cross_transfer = held(self_transfer), held(cross_transfer)
    listing = near_list.transpose(1, 2, 0)
    first = call(
        functools.partial(first_body, axis, count),
        pieces + [pltpu.VMEM((rows, 2 * width), bf16), sent, sent, maps, maps],
        [OFF_CHIP] * 5,
        (held(excitation), held(leaf_basis), self_transfer, cross_transfer, held(listing)),
        8 * rank * rows * width,
        8 * rows * width,
        scratch=[
            pltpu.VMEM(excitation.shape, f32),
            pltpu.VMEM((rank, 2 * rows), bf16),
            pltpu.SMEM(listing.shape, jnp.int32),
            pltpu.SemaphoreType.DMA((13,)),
        ],
    )
    coef = first[:CHUNKS]
    xb, to_pair, to_other, maps0, maps1 = first[CHUNKS:]

    partner = swaps(0, coef)
    pair = lax.ppermute(to_pair, axis, pairs)
    own = own_products(maps0, coef)
    coef = [
        call(
            cross_body,
            [pieces[c]],
            [ON_CHIP] * 3,
            (own[c], partner[c], maps0),
            8 * rank * rank * sizes[c],
            4 * rank * rank,
        )[0]
        for c in range(CHUNKS)
    ]

    partner = swaps(1, coef)
    own = own_products(maps1, coef)
    loaded = rest(0, own[0])
    to_other, *loaded = lax.optimization_barrier((to_other, *loaded))
    other = lax.ppermute(to_other, axis, others)
    coef = [
        call(
            cross_body,
            [pieces[c]],
            [ON_CHIP] * 3,
            (own[c], partner[c], maps1),
            4 * rank * rank * sizes[c],
            2 * rank * rank,
        )[0]
        for c in range(CHUNKS)
    ]
    maps2, basis, tiles = rest(1, coef[0], loaded)
    partner = swaps(2, coef)
    near, side = call(
        functools.partial(near_body, axis, count),
        [pltpu.VMEM((rows, 2 * width), f32), pltpu.VMEM((rows, 4 * tile), bf16)],
        [SCALARS] + [ON_CHIP] * 3,
        (listing, tiles, xb, pair),
        8 * slots * tile * tile * width,
        8 * rows * width,
        scratch=[pltpu.VMEM((slots, tile, 2 * width), bf16)],
    )
    base, fold = call(
        base_body,
        [pltpu.VMEM((rows, 2 * width), f32), pltpu.VMEM((rows, 2 * rank), bf16)],
        [ON_CHIP] * (CHUNKS + 3),
        (*coef, maps2, basis, near),
        8 * rows * rank * (rank + width),
        8 * rows * width,
    )
    whole = jax.ShapeDtypeStruct((2, rows, width), f32)
    scratch = [pltpu.VMEM((rows, width), f32), pltpu.SemaphoreType.DMA((2 * STEPS,))]
    out, left = call(
        last0_body,
        [whole, pltpu.VMEM((rows, width), f32)],
        [ON_CHIP] * 5,
        (partner[0], fold, base, side, other),
        8 * rows * (rank + tile) * width,
        8 * rows * width,
        scratch=scratch,
        outs_at=[OFF_CHIP, ON_CHIP],
    )
    return call(
        last1_body,
        [whole],
        [ON_CHIP] * 3 + [OFF_CHIP],
        (partner[1], fold, left, out),
        2 * rows * rank * width,
        4 * rows * width,
        scratch=scratch,
        outs_at=[OFF_CHIP],
        aliases={3: 0},
    )[0]


def solution(mesh):
    placed = (
        P(None, "surf", None),
        P(None, "surf", None),
        P(None, None, "surf", None),
        P(None, None, "surf", None),
        P(None, "surf", None),
        P("surf", None, None, None),
        P(),
    )
    return jax.shard_map(
        per_device, mesh=mesh, in_specs=placed, out_specs=P(None, "surf", None), check_vma=False
    )
```
